32 devices in a mesh: cp: 16 (over z, y, x), hd: 2 (over core).
Axes of the slice: x: 2, y: 2, z: 4, core: 2. Of those that a mesh axis runs over, the one named last changes fastest.
Arguments:
- queries: bfloat16 [3072, 4096], P('cp', 'hd'), may hold values from -48 to 48
- keys: bfloat16 [3072, 1024], P('cp', 'hd'), may hold values from -48 to 48
- values: bfloat16 [3072, 1024], P('cp', 'hd'), may hold values from -6 to 6
- span_table: int32 [32], replicated, may hold values from 0 to 31, as said below
- doc_ids: int32 [3072], replicated, may hold values from 0 to 7, never falling along the last dimension, each value on 1 to 768 neighbouring positions
- out_weight: bfloat16 [4096, 4096], P('hd'), may hold values from -0.09375 to 0.09375
Outputs:
- mixed: bfloat16 [3072, 4096], P(('cp', 'hd'))
The draws below stay inside these ranges and needn't reach their ends.
Inputs may be any that keep to these rules, and one draw needn't show every extreme that they name: `span_table`: slots 2 j and 2 j + 1 hold two spans c and 31 - c, and every span is held once.
All inputs are finite; a program needn't handle non-finite values.
Results may differ from the reference program's by a relative error of at most 0.0095.
Values may be sent and summed in bfloat16 or wider, within the bound.
A program may use at most 128 MiB of HBM per device.

```python
import math
import jax
import jax.numpy as jnp
import numpy as np
from jax import lax

D = 4096
QUERY_HEADS = 32
KEY_VALUE_HEADS = 8
HEAD_WIDTH = 128
SPAN_TOKENS = 96
DOCS = 8
SPANS = 32
SEQUENCE_TOKENS = 3072


def paired_table(key):
    pairs = jax.random.permutation(jax.random.fold_in(key, 11), SPANS // 2).astype(jnp.int32)
    flips = jax.random.randint(jax.random.fold_in(key, 12), (SPANS // 2,), 0, 2)
    upper = (SPANS - 1 - pairs).astype(jnp.int32)
    first = jnp.where(flips == 1, upper, pairs)
    second = jnp.where(flips == 1, pairs, upper)
    return jnp.stack([first, second], axis=1).reshape(SPANS).astype(jnp.int32)


def draw_span_table(key, part):
    return paired_table(key)


def drawn_pair(key):
    drawn_key_rows = jnp.clip(jax.random.normal(jax.random.fold_in(key, 21), (SEQUENCE_TOKENS, KEY_VALUE_HEADS * HEAD_WIDTH), jnp.float32), -6.0, 6.0)
    base_queries = jnp.clip(jax.random.normal(jax.random.fold_in(key, 22), (SEQUENCE_TOKENS, QUERY_HEADS * HEAD_WIDTH), jnp.float32), -6.0, 6.0)
    new_keys = drawn_key_rows
    new_queries = base_queries
    return (jnp.clip(new_queries, -48.0, 48.0), jnp.clip(new_keys, -48.0, 48.0))


def draw_queries(key, part):
    return drawn_pair(key)[0].astype(jnp.bfloat16)


def draw_keys(key, part):
    return drawn_pair(key)[1].astype(jnp.bfloat16)


def block_levels(rng, dims, shards, smallest, high):
    def one(dim, blocks):
        steps = jax.random.uniform(jax.random.fold_in(jax.random.fold_in(rng, 6), dim), (blocks,), jnp.float32, smallest / len(shards), high / len(shards))
        return jnp.repeat(jnp.exp(steps), dims[dim] // blocks).reshape((-1,) + (1,) * (len(dims) - dim - 1))

    gain = one(*shards[0])
    for cut in shards[1:]:
        gain = gain * one(*cut)
    return gain


def split_up(amount, total, bound, slope):
    portions = [(1 << 20) // math.isqrt(rank ** slope) + 1 for rank in range(2, amount + 1)]
    surplus, given = total - bound - (amount - 1), [1] * (amount - 1)
    while surplus > 0:
        movable = [i for i in range(amount - 1) if given[i] < bound]
        pool, left = sum([portions[i] for i in movable]), surplus
        for i in movable:
            extra = min(bound - given[i], max(1, left * portions[i] // pool), surplus)
            given[i] = given[i] + extra
            surplus = surplus - extra
    return np.array([bound] + given)


def ragged_sizes(own_key, count, total, limit, lean):
    if count == 2:
        one = jax.random.randint(own_key, (), max(1, total - limit), min(limit, total - 1) + 1)
        return jnp.stack([one, total - one])
    sizes = jnp.asarray(split_up(count, total, limit, lean), jnp.int32)
    twos = (count - 1) // 2
    source_of, taker = sizes[1:1 + 2 * twos:2], sizes[2:2 + 2 * twos:2]
    room = jnp.minimum(source_of - 1, limit - taker)
    moved = jax.random.randint(jax.random.fold_in(own_key, 1), (twos,), 0, 1 << 20) % (room + 1)
    sizes = sizes.at[1:1 + 2 * twos:2].set(source_of - moved).at[2:2 + 2 * twos:2].set(taker + moved)
    return sizes[jax.random.permutation(jax.random.fold_in(own_key, 2), count)]


def centred(key, dims, width, bound, cuts=(), kind=jnp.bfloat16):
    gain = block_levels(key, dims, cuts, -0.22, 0.18) if cuts else 1.0
    values = jax.random.normal(key, dims, jnp.float32) * width * gain
    return jnp.minimum(jnp.maximum(values, -bound), bound).astype(kind)


def setup_inputs(seed: int = 0) -> dict:
    seeds = jax.random.split(jax.random.key(seed), 7)
    return {
        "queries": draw_queries(jax.random.fold_in(seeds[6], 71), 0),
        "keys": draw_keys(jax.random.fold_in(seeds[6], 71), 0),
        "values": centred(seeds[2], (SEQUENCE_TOKENS, KEY_VALUE_HEADS * HEAD_WIDTH), 1.0, 6.0, ((0, 16), (1, 2))),
        "span_table": draw_span_table(jax.random.fold_in(seeds[6], 71), 0),
        "doc_ids": jnp.searchsorted(jnp.cumsum(ragged_sizes(seeds[4], DOCS, SEQUENCE_TOKENS, SEQUENCE_TOKENS // 4, 2)), jnp.arange(SEQUENCE_TOKENS), side="right").astype(jnp.int32),
        "out_weight": centred(seeds[5], (QUERY_HEADS * HEAD_WIDTH, D), (QUERY_HEADS * HEAD_WIDTH) ** -0.5, 0.09375, ((0, 2),)),
    }


def reference(queries, keys, values, span_table, doc_ids, out_weight):
    query_group = QUERY_HEADS // KEY_VALUE_HEADS
    scale = HEAD_WIDTH ** -0.5
    rows = jnp.arange(SEQUENCE_TOKENS, dtype=jnp.int32)
    positions = (span_table[rows // SPAN_TOKENS] * SPAN_TOKENS + rows % SPAN_TOKENS).astype(jnp.int32)
    documents = doc_ids[positions]
    key_head_rows = keys.reshape(SEQUENCE_TOKENS, KEY_VALUE_HEADS, HEAD_WIDTH).astype(jnp.float32)
    value_head_rows = values.reshape(SEQUENCE_TOKENS, KEY_VALUE_HEADS, HEAD_WIDTH).astype(jnp.float32)

    def block(index):
        first = (index * SPAN_TOKENS).astype(jnp.int32)
        query_matrix = lax.dynamic_slice_in_dim(queries, first, SPAN_TOKENS, 0)
        query_matrix = query_matrix.reshape(SPAN_TOKENS, KEY_VALUE_HEADS, query_group, HEAD_WIDTH).astype(jnp.float32)
        query_pos = lax.dynamic_slice_in_dim(positions, first, SPAN_TOKENS, 0)
        query_doc = lax.dynamic_slice_in_dim(documents, first, SPAN_TOKENS, 0)
        visible = (positions[None, :] <= query_pos[:, None]) & (documents[None, :] == query_doc[:, None])
        scores = jnp.einsum("qkgd,nkd->kgqn", query_matrix, key_head_rows) * scale
        scores = jnp.where(visible, scores, -1e30)
        best = jnp.max(scores, axis=-1, keepdims=True)
        weights = jnp.where(visible, jnp.exp(scores - best), 0.0)
        denom = jnp.sum(weights, axis=-1)
        rounded = lax.optimization_barrier(weights.astype(jnp.bfloat16)).astype(jnp.float32)
        numer = jnp.einsum("kgqn,nkd->kgqd", rounded, value_head_rows)
        result = numer / denom[..., None]
        return result.transpose(2, 0, 1, 3).reshape(SPAN_TOKENS, QUERY_HEADS * HEAD_WIDTH).astype(jnp.bfloat16)

    attn = lax.map(block, jnp.arange(SEQUENCE_TOKENS // SPAN_TOKENS, dtype=jnp.int32)).reshape(SEQUENCE_TOKENS, QUERY_HEADS * HEAD_WIDTH)
    return jnp.dot(attn, out_weight, preferred_element_type=jnp.float32).astype(jnp.bfloat16)
```

```python
import functools
import math

import jax
import jax.numpy as jnp
from jax import lax
from jax.experimental import pallas as pl
from jax.experimental.pallas import tpu as pltpu
from jax.sharding import PartitionSpec as P

HEAD_WIDTH = 128
DOCS = 8
LANES = 256
MATES = 4
NEG = -1e30
MESH = pl.DeviceIdType.MESH
FACTOR = HEAD_WIDTH ** (-0.5) * math.log2(math.e)
f32, bf16 = jnp.float32, jnp.bfloat16


def kernel(
    line, span_ref, doc_ref, q_hbm, k_hbm, v_hbm, w_hbm, out_ref,
    kv, kv_out, q_in, q_out, marks, q_t, acc, best, total, fades, held,
    w_vmem, attn, o_out, outgoing, incoming, kept,
    load_kv, load_q, w_sem, send_kv, send_q, send_o, send_z, recv_kv, recv_q, recv_o, out_send, out_recv,
):
    rows = k_hbm.shape[0]
    span_len = rows // 2
    wide = q_hbm.shape[1] // MATES
    group = wide // HEAD_WIDTH
    tiles = group * rows // LANES
    me = lax.axis_index("cp")
    hd = lax.axis_index("hd")
    z, p = me // MATES, me % MATES
    y, x = p // 2, p % 2
    has_up, has_down = z < line - 1, z > 0
    up, down = me + MATES, me - MATES

    def member(i):
        return (y + (i // 2) * (1 - 2 * y)) * 2 + x + (i % 2) * (1 - 2 * x)

    def mate(i):
        return z * MATES + member(i)

    def columns(i, size):
        return pl.ds(pl.multiple_of(member(i) * size, size), size)

    def kv_load(i, h):
        src = (k_hbm, v_hbm)[h].at[:, columns(i, HEAD_WIDTH)]
        dst = kv.at[me, h] if i == 0 else kv_out.at[i, h]
        return pltpu.make_async_copy(src, dst, load_kv.at[i, h])

    def q_load(i):
        dst = q_in.at[0] if i == 0 else q_out.at[i]
        return pltpu.make_async_copy(q_hbm.at[:, columns(i, wide)], dst, load_q.at[i])

    def w_load(i):
        src = w_hbm.at[pl.ds(pl.multiple_of(member(i) * wide, wide), wide), :]
        return pltpu.make_async_copy(src, w_vmem.at[i * wide:(i + 1) * wide, :], w_sem.at[i])

    def remote(src, dst, send, recv, target):
        return pltpu.make_async_remote_copy(
            src_ref=src, dst_ref=dst, send_sem=send, recv_sem=recv,
            device_id={"cp": target}, device_id_type=MESH,
        )

    def kv_send(i, h):
        return remote(kv_out.at[i, h], kv.at[me, h], send_kv.at[i, h], recv_kv.at[me, h], mate(i))

    def q_send(i):
        return remote(q_out.at[i], q_in.at[i], send_q.at[i], recv_q.at[i], mate(i))

    def o_send(i):
        dst = attn.at[:, pl.ds(pl.multiple_of(i * wide, wide), wide)]
        return remote(o_out.at[i], dst, send_o.at[i], recv_o.at[i], mate(i))

    def z_send(d, side, i, h, src, target):
        block = kv.at[src, h]
        return remote(block, block, send_z.at[d, side, i, h], recv_kv.at[src, h], target)

    def arrived(src):
        for h in range(2):
            remote(kv.at[src, h], kv.at[src, h], send_z.at[0, 0, 0, h], recv_kv.at[src, h], mate(1)).wait_recv()

    for i in range(MATES):
        for h in range(2):
            kv_load(i, h).start()
    for i in range(MATES):
        q_load(i).start()

    barrier = pltpu.get_barrier_semaphore()
    for i in range(1, MATES):
        pl.semaphore_signal(barrier, inc=1, device_id={"cp": mate(i)}, device_id_type=MESH)
    pl.semaphore_signal(barrier, inc=1, device_id={"hd": 1 - hd}, device_id_type=MESH)

    @pl.when(has_up)
    def _():
        pl.semaphore_signal(barrier, inc=1, device_id={"cp": up}, device_id_type=MESH)

    @pl.when(has_down)
    def _():
        pl.semaphore_signal(barrier, inc=1, device_id={"cp": down}, device_id_type=MESH)

    for h in range(2):
        kv_load(0, h).wait()
    pl.semaphore_wait(barrier, MATES + has_up.astype(jnp.int32) + has_down.astype(jnp.int32))

    def own_z(i, h, act):
        @pl.when(has_up)
        def _():
            act(z_send(0, 0, i, h, mate(i), up))

        @pl.when(has_down)
        def _():
            act(z_send(0, 1, i, h, mate(i), down))

    def go(copy):
        copy.start()

    def sent(copy):
        copy.wait_send()

    for h in range(2):
        own_z(0, h, go)
    for i in range(1, MATES):
        for h in range(2):
            kv_load(i, h).wait()
            kv_send(i, h).start()
    for i in range(1, MATES):
        q_load(i).wait()
        q_send(i).start()
    for i in range(MATES):
        w_load(i).start()

    docs = doc_ref[...]
    starts = [jnp.zeros((1, 1), f32)]
    for d in range(1, DOCS):
        starts.append(jnp.sum(jnp.where(docs < d, 1.0, 0.0), keepdims=True))
    starts.append(jnp.full((1, 1), docs.size, f32))
    lane = lax.broadcasted_iota(jnp.int32, (1, HEAD_WIDTH), 1)
    start_row = jnp.full((1, HEAD_WIDTH), 4.0 * docs.size, f32)
    end_row = jnp.full((1, HEAD_WIDTH), 4.0 * docs.size, f32)
    for d in range(DOCS):
        start_row = jnp.where(lane == d, starts[d], start_row)
        end_row = jnp.where(lane == d, starts[d + 1], end_row)
    span_row = jnp.full((1, HEAD_WIDTH), docs.size, jnp.int32)
    for i in range(MATES):
        for s in range(2):
            span_row = jnp.where(lane == DOCS + 2 * i + s, span_ref[2 * mate(i) + s], span_row)

    def mark(src):
        key = lax.broadcasted_iota(jnp.int32, (rows, HEAD_WIDTH), 0)
        first = key < span_len
        span = jnp.where(first, span_ref[2 * src], span_ref[2 * src + 1])
        key_pos = (span * span_len + jnp.where(first, key, key - span_len)).astype(f32)
        of_doc = jnp.where((key_pos >= start_row) & (key_pos < end_row), 1.0, 0.0)
        marks[src] = jnp.where(span > span_row, NEG, of_doc).astype(bf16)

    def q_place(i):
        at = lax.broadcasted_iota(jnp.int32, (1, group * rows), 1) % rows
        s0, s1 = span_ref[2 * mate(i)], span_ref[2 * mate(i) + 1]
        pos = jnp.where(at < span_len, s0 * span_len + at, (s1 - 1) * span_len + at)
        return at, pos.astype(f32)

    def prepare(i):
        heads = [q_in[i, :, h * HEAD_WIDTH:(h + 1) * HEAD_WIDTH] for h in range(group)]
        flipped = jnp.concatenate(heads, axis=0).T
        at, pos = q_place(i)
        row = lax.broadcasted_iota(jnp.int32, (HEAD_WIDTH, group * rows), 0)
        extra = jnp.where(row == DOCS + 2 * i + (at >= span_len).astype(jnp.int32), 1.0, 0.0)
        for d in range(DOCS):
            same = (pos >= starts[d]) & (pos < starts[d + 1])
            extra = jnp.where(row == d, jnp.where(same, 0.0, NEG), extra)
        extra = extra.astype(bf16)
        for c in range(tiles):
            cut = slice(c * LANES, (c + 1) * LANES)
            q_t[i, c, :HEAD_WIDTH] = flipped[:, cut]
            q_t[i, c, HEAD_WIDTH:] = extra[:, cut]
            acc[i, c] = jnp.zeros((HEAD_WIDTH, LANES), f32)
            total[i, c] = jnp.zeros((1, LANES), f32)
            best[i, c] = jnp.full((1, LANES), NEG, f32)

    def attend(i, plane, own=False):
        base = plane * MATES
        if own:
            _, pos = q_place(i)

        def weigh(c):
            parts = []
            for b in range(MATES):
                src = base + b
                keys = jnp.concatenate([kv[src, 0], marks[src]], axis=1)
                scores = jnp.dot(keys, q_t[i, c], preferred_element_type=f32)
                if own:
                    key = lax.broadcasted_iota(jnp.int32, (rows, LANES), 0)
                    key_pos = jnp.where(
                        key < span_len, span_ref[2 * src] * span_len, (span_ref[2 * src + 1] - 1) * span_len
                    ) + key
                    late = key_pos.astype(f32) > pos[:, c * LANES:(c + 1) * LANES]
                    scores = jnp.where(late, NEG, scores)
                parts.append(scores)
            tops = [jnp.max(s, axis=0, keepdims=True) for s in parts]
            old = best[i, c]
            top = functools.reduce(jnp.maximum, tops, old)
            fade = jnp.exp2((old - top) * FACTOR)
            shift = top * FACTOR
            summed = total[i, c] * fade
            for b, scores in enumerate(parts):
                weights = jnp.exp2(scores * FACTOR - shift)
                summed = summed + jnp.sum(weights, axis=0, keepdims=True)
                held[c, b * rows:(b + 1) * rows] = weights.astype(bf16)
            total[i, c] = summed
            best[i, c] = top
            fades[c] = fade

        values = jnp.concatenate([kv[base + b, 1] for b in range(MATES)], axis=0).T

        def gather(c):
            part = jnp.dot(values, held[c], preferred_element_type=f32)
            acc[i, c] = acc[i, c] * fades[c] + part

        for c in range(tiles):
            weigh(c)
            if c:
                gather(c - 1)
        gather(tiles - 1)

    def finalize(i):
        parts = [acc[i, c] / total[i, c] for c in range(tiles)]
        turned = jnp.concatenate(parts, axis=1).T.astype(bf16)
        for h in range(group):
            o_out[i, :, h * HEAD_WIDTH:(h + 1) * HEAD_WIDTH] = turned[h * rows:(h + 1) * rows]

    def forward(d, i):
        for side, plane, more, target in ((0, z - d, has_up, up), (1, z + d, has_down, down)):
            src = plane * MATES + member(i)

            @pl.when((plane >= 0) & (plane < line))
            def _():
                arrived(src)

                @pl.when(more)
                def _():
                    for h in range(2):
                        z_send(d, side, i, h, src, target).start()

    def drained(d, i):
        for side, plane, more, target in ((0, z - d, has_up, up), (1, z + d, has_down, down)):
            src = plane * MATES + member(i)

            @pl.when(jnp.minimum(jnp.minimum(plane, line - 1 - plane), more.astype(jnp.int32) - 1) >= 0)
            def _():
                for h in range(2):
                    z_send(d, side, i, h, src, target).wait_send()

    q_load(0).wait()
    prepare(0)
    for i in range(1, MATES):
        for h in range(2):
            kv_send(i, h).wait_send()
        arrived(mate(i))
        for h in range(2):
            own_z(i, h, go)

    def mark_step(src, carry):
        mark(src)
        return carry

    lax.fori_loop(0, line * MATES, mark_step, 0)
    attend(0, z, own=True)
    for i in range(MATES):
        forward(1, i)

    def own_step(i, carry):
        q_send(i).wait_recv()
        prepare(i)
        attend(i, z, own=True)
        return carry

    lax.fori_loop(1, MATES, own_step, 0)

    furthest = jnp.maximum(z, line - 1 - z)

    def step(n, carry):
        d, k = n // MATES + 1, n % MATES
        i = MATES - 1 - k

        @pl.when(d < line - 1)
        def _():
            forward(d + 1, k)

        def side(s, inner):
            plane = z + d * (2 * s - 1)

            @pl.when((plane >= 0) & (plane < line))
            def _():
                attend(i, plane)

            return inner

        lax.fori_loop(0, 2, side, 0)

        @pl.when(d == furthest)
        def _():
            finalize(i)

            @pl.when(i > 0)
            def _():
                o_send(i).start()

        return carry

    lax.fori_loop(0, (line - 1) * MATES, step, 0)

    attn[:, :wide] = o_out[0]
    for i in range(MATES):
        w_load(i).wait()
    for i in range(1, MATES):
        o_send(i).wait_recv()

    half = rows // 2
    count, width = outgoing.shape[0], outgoing.shape[2]

    def hand_over(n):
        return pltpu.make_async_remote_copy(
            src_ref=outgoing.at[n], dst_ref=incoming.at[n], send_sem=out_send.at[n],
            recv_sem=out_recv.at[n], device_id={"hd": 1 - hd}, device_id_type=MESH,
        )

    @pl.loop(0, count)
    def _(n):
        cols = pl.ds(pl.multiple_of(n * width, width), width)
        product = jnp.dot(attn[...], w_vmem[:, cols], preferred_element_type=f32)
        upper, lower = product[:half], product[half:]
        mine = hd == 0
        outgoing[n] = jnp.where(mine, lower, upper).astype(bf16)
        kept[n] = jnp.where(mine, upper, lower)
        hand_over(n).start()

    for n in range(count):
        hand_over(n).wait_recv()
        out_ref[:, n * width:(n + 1) * width] = (kept[n] + incoming[n].astype(f32)).astype(bf16)

    for n in range(count):
        hand_over(n).wait_send()
    for i in range(1, MATES):
        q_send(i).wait_send()
        o_send(i).wait_send()
    for i in range(MATES):
        for h in range(2):
            own_z(i, h, sent)

    def drain(n, carry):
        drained(n // MATES + 1, n % MATES)
        return carry

    lax.fori_loop(0, (line - 1) * MATES, drain, 0)


def local(cp, queries, keys, values, span_table, doc_ids, out_weight):
    rows = queries.shape[0]
    kv_heads = keys.shape[1] // HEAD_WIDTH
    wide = queries.shape[1] // kv_heads
    tiles = wide // HEAD_WIDTH * rows // LANES
    line = cp // MATES
    model = out_weight.shape[1]
    count = 8
    width = model // count
    half = rows // 2
    vmem, hbm = pltpu.VMEM, pl.ANY
    spec = lambda space: pl.BlockSpec(memory_space=space)
    dma = pltpu.SemaphoreType.DMA
    return pl.pallas_call(
        functools.partial(kernel, line),
        out_shape=jax.ShapeDtypeStruct((half, model), bf16),
        in_specs=[spec(pltpu.SMEM), spec(vmem), spec(hbm), spec(hbm), spec(hbm), spec(hbm)],
        out_specs=spec(vmem),
        scratch_shapes=[
            vmem((cp, 2, rows, HEAD_WIDTH), bf16),
            vmem((MATES, 2, rows, HEAD_WIDTH), bf16),
            vmem((MATES, rows, wide), bf16),
            vmem((MATES, rows, wide), bf16),
            vmem((cp, rows, HEAD_WIDTH), bf16),
            vmem((MATES, tiles, 2 * HEAD_WIDTH, LANES), bf16),
            vmem((MATES, tiles, HEAD_WIDTH, LANES), f32),
            vmem((MATES, tiles, 1, LANES), f32),
            vmem((MATES, tiles, 1, LANES), f32),
            vmem((tiles, 1, LANES), f32),
            vmem((tiles, MATES * rows, LANES), bf16),
            vmem(out_weight.shape, bf16),
            vmem((rows, MATES * wide), bf16),
            vmem((MATES, rows, wide), bf16),
            vmem((count, half, width), bf16),
            vmem((count, half, width), bf16),
            vmem((count, half, width), f32),
            dma((MATES, 2)), dma((MATES,)), dma((MATES,)), dma((MATES, 2)), dma((MATES,)), dma((MATES,)),
            dma((line, 2, MATES, 2)), dma((cp, 2)), dma((MATES,)), dma((MATES,)), dma((count,)), dma((count,)),
        ],
        compiler_params=pltpu.CompilerParams(
            collective_id=0, has_side_effects=True, vmem_limit_bytes=62 * 2 ** 20,
        ),
    )(span_table, doc_ids.reshape(-1, 128), queries, keys, values, out_weight)


def solution(mesh):
    return jax.shard_map(
        functools.partial(local, mesh.shape["cp"]),
        mesh=mesh,
        in_specs=(P("cp", "hd"), P("cp", "hd"), P("cp", "hd"), P(), P(), P("hd", None)),
        out_specs=P(("cp", "hd"), None),
        check_vma=False,
    )
```

```python
import functools
import math

import jax
import jax.numpy as jnp
from jax import lax
from jax.experimental import pallas as pl
from jax.experimental.pallas import tpu as pltpu
from jax.sharding import PartitionSpec as P

HEAD_WIDTH = 128
DOCS = 8
MATES = 4
DOCUMENT_SHARE = 4
NEG = -1e30
MESH = pl.DeviceIdType.MESH
FACTOR = HEAD_WIDTH ** (-0.5) * math.log2(math.e)
f32, bf16 = jnp.float32, jnp.bfloat16


def kernel(
    line, span_ref, doc_ref, q_hbm, k_hbm, v_hbm, w_hbm, out_ref,
    kv, kv_out, q_in, q_out, marks, q_t, slot_of, k_near, v_near, raw, held,
    w_vmem, attn, o_out, partial, outgoing, incoming, kept,
    load_kv, load_q, w_sem, send_kv, send_q, send_o, send_z, recv_kv, recv_q, recv_o, out_send, out_recv, turn,
):
    rows = k_hbm.shape[0]
    span_len = rows // 2
    wide = q_hbm.shape[1] // MATES
    group = wide // HEAD_WIDTH
    slots = span_ref.shape[0]
    reach = k_near.shape[1] // span_len
    me = lax.axis_index("cp")
    hd = lax.axis_index("hd")
    z, p = me // MATES, me % MATES
    y, x = p // 2, p % 2
    has_up, has_down = z < line - 1, z > 0
    up, down = me + MATES, me - MATES

    def member(i):
        return (y + (i // 2) * (1 - 2 * y)) * 2 + x + (i % 2) * (1 - 2 * x)

    def mate(i):
        return z * MATES + member(i)

    def columns(i, size):
        return pl.ds(pl.multiple_of(member(i) * size, size), size)

    class kv_load:
        def __init__(self, i, h):
            spot = kv.at[me, h] if i == 0 else kv_out.at[i, h]
            self.copies = [
                pltpu.make_async_copy(
                    (k_hbm, v_hbm)[h].at[s * span_len:(s + 1) * span_len, columns(i, HEAD_WIDTH)],
                    spot.at[s], load_kv.at[i, h, s],
                )
                for s in range(2)
            ]

        def start(self):
            for copy in self.copies:
                copy.start()

        def wait(self):
            for copy in self.copies:
                copy.wait()

    def q_load(i):
        dst = q_in.at[0] if i == 0 else q_out.at[i]
        return pltpu.make_async_copy(q_hbm.at[:, columns(i, wide)], dst, load_q.at[i])

    def w_load(i):
        src = w_hbm.at[pl.ds(pl.multiple_of(member(i) * wide, wide), wide), :]
        return pltpu.make_async_copy(src, w_vmem.at[i * wide:(i + 1) * wide, :], w_sem.at[i])

    def remote(src, dst, send, recv, target):
        return pltpu.make_async_remote_copy(
            src_ref=src, dst_ref=dst, send_sem=send, recv_sem=recv,
            device_id={"cp": target}, device_id_type=MESH,
        )

    def kv_send(i, h):
        return remote(kv_out.at[i, h], kv.at[me, h], send_kv.at[i, h], recv_kv.at[me, h], mate(i))

    def q_send(i):
        return remote(q_out.at[i], q_in.at[i], send_q.at[i], recv_q.at[i], mate(i))

    def o_send(i):
        dst = attn.at[:, pl.ds(pl.multiple_of(i * wide, wide), wide)]
        return remote(o_out.at[i], dst, send_o.at[i], recv_o.at[i], mate(i))

    def z_send(d, side, i, h, src, target):
        block = kv.at[src, h]
        return remote(block, block, send_z.at[d, side, i, h], recv_kv.at[src, h], target)

    def z_block(d, side, i, src, target):
        return remote(kv.at[src], kv.at[src], send_z.at[d, side, i, 0], recv_kv.at[src, 0], target)

    def arrived(d, src):
        @pl.when(d == 1)
        def _():
            for h in range(2):
                remote(kv.at[src, h], kv.at[src, h], send_z.at[0, 0, 0, h], recv_kv.at[src, h], mate(1)).wait_recv()

        @pl.when(d > 1)
        def _():
            z_block(0, 0, 0, src, mate(1)).wait_recv()

    for i in range(MATES):
        for h in range(2):
            kv_load(i, h).start()
    for i in range(MATES):
        q_load(i).start()

    barrier = pltpu.get_barrier_semaphore()
    for i in range(1, MATES):
        pl.semaphore_signal(barrier, inc=1, device_id={"cp": mate(i)}, device_id_type=MESH)
    pl.semaphore_signal(barrier, inc=1, device_id={"hd": 1 - hd}, device_id_type=MESH)

    @pl.when(has_up)
    def _():
        pl.semaphore_signal(barrier, inc=1, device_id={"cp": up}, device_id_type=MESH)

    @pl.when(has_down)
    def _():
        pl.semaphore_signal(barrier, inc=1, device_id={"cp": down}, device_id_type=MESH)

    for h in range(2):
        kv_load(0, h).wait()
    pl.semaphore_wait(barrier, MATES + has_up.astype(jnp.int32) + has_down.astype(jnp.int32))

    def own_z(i, h, act):
        @pl.when(has_up)
        def _():
            act(z_send(0, 0, i, h, mate(i), up))

        @pl.when(has_down)
        def _():
            act(z_send(0, 1, i, h, mate(i), down))

    def go(copy):
        copy.start()

    def sent(copy):
        copy.wait_send()

    for h in range(2):
        own_z(0, h, go)
    for i in range(1, MATES):
        for h in range(2):
            kv_load(i, h).wait()
            kv_send(i, h).start()

    def send_queries():
        for i in range(1, MATES):
            q_load(i).wait()
            q_send(i).start()

    @pl.when(hd == 0)
    def _():
        send_queries()


    docs = doc_ref[...]
    starts = [jnp.zeros((1, 1), f32)]
    for d in range(1, DOCS):
        starts.append(jnp.sum(jnp.where(docs < d, 1.0, 0.0), keepdims=True))
    starts.append(jnp.full((1, 1), docs.size, f32))
    lane = lax.broadcasted_iota(jnp.int32, (1, HEAD_WIDTH), 1)
    start_row = jnp.full((1, HEAD_WIDTH), 4.0 * docs.size, f32)
    end_row = jnp.full((1, HEAD_WIDTH), 4.0 * docs.size, f32)
    for d in range(DOCS):
        start_row = jnp.where(lane == d, starts[d], start_row)
        end_row = jnp.where(lane == d, starts[d + 1], end_row)
    void = jnp.where(lane == DOCS, NEG, 0.0)
    marks[slots] = jnp.broadcast_to(void, (span_len, HEAD_WIDTH)).astype(bf16)

    def mark(slot, carry):
        key = lax.broadcasted_iota(jnp.int32, (span_len, HEAD_WIDTH), 0)
        key_pos = (span_ref[slot] * span_len + key).astype(f32)
        of_doc = jnp.where((key_pos >= start_row) & (key_pos < end_row), 1.0, 0.0)
        marks[slot] = of_doc.astype(bf16)
        found = 0
        for other in range(slots):
            found = jnp.maximum(found, jnp.where(span_ref[other] == slot, other, 0))
        slot_of[slot] = found
        return carry

    lanes = group * span_len

    def prepare(i):
        at = lax.broadcasted_iota(jnp.int32, (1, lanes), 1) % span_len
        row = lax.broadcasted_iota(jnp.int32, (HEAD_WIDTH, lanes), 0)
        for s in range(2):
            heads = [
                q_in[i, s * span_len:(s + 1) * span_len, h * HEAD_WIDTH:(h + 1) * HEAD_WIDTH]
                for h in range(group)
            ]
            pos = (span_ref[2 * mate(i) + s] * span_len + at).astype(f32)
            extra = jnp.where(row == DOCS, 1.0, 0.0)
            for d in range(DOCS):
                same = (pos >= starts[d]) & (pos < starts[d + 1])
                extra = jnp.where(row == d, jnp.where(same, 0.0, NEG), extra)
            q_t[2 * i + s, :HEAD_WIDTH] = jnp.concatenate(heads, axis=0).T
            q_t[2 * i + s, HEAD_WIDTH:] = extra.astype(bf16)

    turns = [(i, s) for i in (3, 1, 2, 0) for s in range(2)]
    tops = {}

    def collect(j):
        i, s = turns[j]
        last = span_ref[2 * mate(i) + s]
        for k in range(reach):
            span = last - (reach - 1) + k
            slot = slot_of[jnp.maximum(span, 0)]
            cut = slice(k * span_len, (k + 1) * span_len)
            k_near[j % 2, cut, :HEAD_WIDTH] = kv[slot // 2, 0, slot % 2]
            k_near[j % 2, cut, HEAD_WIDTH:] = marks[jnp.where(span >= 0, slot, slots)]
            v_near[j % 2, cut] = kv[slot // 2, 1, slot % 2]

    def score(j):
        i, s = turns[j]
        scores = jnp.dot(k_near[j % 2], q_t[2 * i + s], preferred_element_type=f32)
        edge = (reach - 1) * span_len
        key = lax.broadcasted_iota(jnp.int32, (span_len, lanes), 0)
        at = lax.broadcasted_iota(jnp.int32, (span_len, lanes), 1) % span_len
        corner = jnp.where(key > at, NEG, scores[edge:])
        raw[j % 2, :edge] = scores[:edge]
        raw[j % 2, edge:] = corner
        top = jnp.max(corner, axis=0, keepdims=True)
        tops[j] = jnp.maximum(top, jnp.max(scores[:edge], axis=0, keepdims=True))

    def weigh(j):
        weights = jnp.exp2(raw[j % 2] * FACTOR - tops[j] * FACTOR)
        tops[j] = 1.0 / jnp.sum(weights, axis=0, keepdims=True)
        held[j % 2] = weights.astype(bf16)

    def blend(j):
        i, s = turns[j]
        mixed = jnp.dot(v_near[j % 2].T, held[j % 2], preferred_element_type=f32)
        turned = (mixed * tops[j]).astype(bf16).T
        for h in range(group):
            o_out[i, s * span_len:(s + 1) * span_len, h * HEAD_WIDTH:(h + 1) * HEAD_WIDTH] = (
                turned[h * span_len:(h + 1) * span_len]
            )
        if s and i:
            o_send(i).start()

    ways = ((0, -1, z, has_up, up), (1, 1, line - 1 - z, has_down, down))

    def forward(d, i):
        for side, sign, last, more, target in ways:
            src = (z + sign * d) * MATES + member(i)

            @pl.when(d <= last)
            def _():
                arrived(d, src)

                @pl.when(more)
                def _():
                    z_block(d, side, i, src, target).start()

    def await_turn():
        for side, sign, last, more, target in ways:

            @pl.when(jnp.minimum(last, more.astype(jnp.int32)) > 0)
            def _():
                pl.semaphore_wait(turn.at[side], 1)

    def give_turn(d):
        for side, sign, last, more, target in ways:
            src = (z + sign * d) * MATES + member(MATES - 1)

            @pl.when((last == d) & more)
            def _():
                z_block(d, side, MATES - 1, src, target).wait_send()
                pl.semaphore_signal(turn.at[side], inc=1, device_id={"hd": 1 - hd}, device_id_type=MESH)

    def drained(d, i):
        for side, sign, last, more, target in ways:
            src = (z + sign * d) * MATES + member(i)
            waited = jnp.maximum(jnp.maximum(hd, MATES - 1 - i), last - d) == 0

            @pl.when((d <= last) & more & jnp.logical_not(waited))
            def _():
                z_block(d, side, i, src, target).wait_send()

    def pass_on(i, h):
        src = mate(i)
        remote(kv.at[src, h], kv.at[src, h], send_z.at[0, 0, 0, h], recv_kv.at[src, h], src).wait_recv()
        own_z(i, h, go)

    def relay(n, carry):
        forward(n // MATES + 1, n % MATES)
        return carry

    for h in range(2):
        pass_on(1, h)
        pass_on(2, h)
    for i in range(MATES):
        w_load(i).start()
    for h in range(2):
        pass_on(3, h)

    @pl.when(hd == 0)
    def _():
        lax.fori_loop(0, (line - 1) * MATES, relay, 0)
        for d in range(1, line):
            give_turn(d)

    @pl.when(hd == 1)
    def _():
        send_queries()

    lax.fori_loop(0, slots, mark, 0)
    q_load(0).wait()
    prepare(0)
    for i in range(1, MATES):
        q_send(i).wait_recv()
        prepare(i)

    @pl.when(hd == 1)
    def _():
        await_turn()
        lax.fori_loop(0, (line - 1) * MATES, relay, 0)

    collect(0)
    score(0)
    for j in range(len(turns)):
        if j + 1 < len(turns):
            collect(j + 1)
            score(j + 1)
        weigh(j)
        blend(j)

    attn[:, :wide] = o_out[0]
    for i in range(MATES):
        w_load(i).wait()

    half = rows // 2
    count, width = outgoing.shape[0], outgoing.shape[2]

    def hand_over(n):
        return pltpu.make_async_remote_copy(
            src_ref=outgoing.at[n], dst_ref=incoming.at[n], send_sem=out_send.at[n],
            recv_sem=out_recv.at[n], device_id={"hd": 1 - hd}, device_id_type=MESH,
        )

    def project(n, i):
        cut = slice(i * wide, (i + 1) * wide)
        return jnp.dot(attn[:, cut], w_vmem[cut, n * width:(n + 1) * width], preferred_element_type=f32)

    for n in range(count):
        partial[n] = project(n, 0)
    for i in (3, 1):
        o_send(i).wait_recv()
        for n in range(count):
            partial[n] += project(n, i)
    o_send(2).wait_recv()
    mine = hd == 0
    for n in range(count):
        product = partial[n] + project(n, 2)
        upper, lower = product[:half], product[half:]
        outgoing[n] = jnp.where(mine, lower, upper).astype(bf16)
        kept[n] = jnp.where(mine, upper, lower)
        hand_over(n).start()

    for n in range(count):
        hand_over(n).wait_recv()
        out_ref[:, n * width:(n + 1) * width] = (kept[n] + incoming[n].astype(f32)).astype(bf16)

    for n in range(count):
        hand_over(n).wait_send()
    for i in range(1, MATES):
        for h in range(2):
            kv_send(i, h).wait_send()
        q_send(i).wait_send()
        o_send(i).wait_send()
    for i in range(MATES):
        for h in range(2):
            own_z(i, h, sent)

    def drain(n, carry):
        drained(n // MATES + 1, n % MATES)
        return carry

    lax.fori_loop(0, (line - 1) * MATES, drain, 0)


def local(cp, queries, keys, values, span_table, doc_ids, out_weight):
    rows = queries.shape[0]
    kv_heads = keys.shape[1] // HEAD_WIDTH
    wide = queries.shape[1] // kv_heads
    slots = span_table.shape[0]
    span_len = rows // 2
    lanes = wide // HEAD_WIDTH * span_len
    near = (slots // DOCUMENT_SHARE + 1) * span_len
    line = cp // MATES
    model = out_weight.shape[1]
    count = 8
    width = model // count
    half = rows // 2
    vmem, hbm = pltpu.VMEM, pl.ANY
    spec = lambda space: pl.BlockSpec(memory_space=space)
    dma = pltpu.SemaphoreType.DMA
    return pl.pallas_call(
        functools.partial(kernel, line),
        out_shape=jax.ShapeDtypeStruct((half, model), bf16),
        in_specs=[spec(pltpu.SMEM), spec(vmem), spec(hbm), spec(hbm), spec(hbm), spec(hbm)],
        out_specs=spec(vmem),
        scratch_shapes=[
            vmem((cp, 2, 2, span_len, HEAD_WIDTH), bf16),
            vmem((MATES, 2, 2, span_len, HEAD_WIDTH), bf16),
            vmem((MATES, rows, wide), bf16),
            vmem((MATES, rows, wide), bf16),
            vmem((slots + 1, span_len, HEAD_WIDTH), bf16),
            vmem((2 * MATES, 2 * HEAD_WIDTH, lanes), bf16),
            pltpu.SMEM((slots,), jnp.int32),
            vmem((2, near, 2 * HEAD_WIDTH), bf16),
            vmem((2, near, HEAD_WIDTH), bf16),
            vmem((2, near, lanes), f32),
            vmem((2, near, lanes), bf16),
            vmem(out_weight.shape, bf16),
            vmem((rows, MATES * wide), bf16),
            vmem((MATES, rows, wide), bf16),
            vmem((count, rows, width), f32),
            vmem((count, half, width), bf16),
            vmem((count, half, width), bf16),
            vmem((count, half, width), f32),
            dma((MATES, 2, 2)), dma((MATES,)), dma((MATES,)), dma((MATES, 2)), dma((MATES,)), dma((MATES,)),
            dma((line, 2, MATES, 2)), dma((cp, 2)), dma((MATES,)), dma((MATES,)), dma((count,)), dma((count,)),
            pltpu.SemaphoreType.REGULAR((2,)),
        ],
        compiler_params=pltpu.CompilerParams(
            collective_id=0, has_side_effects=True, vmem_limit_bytes=62 * 2 ** 20,
        ),
    )(span_table, doc_ids.reshape(-1, 128), queries, keys, values, out_weight)


def solution(mesh):
    return jax.shard_map(
        functools.partial(local, mesh.shape["cp"]),
        mesh=mesh,
        in_specs=(P("cp", "hd"), P("cp", "hd"), P("cp", "hd"), P(), P(), P("hd", None)),
        out_specs=P(("cp", "hd"), None),
        check_vma=False,
    )
```

```python
import functools
import math

import jax
import jax.numpy as jnp
from jax import lax
from jax.experimental import pallas as pl
from jax.experimental.pallas import tpu as pltpu
from jax.sharding import PartitionSpec as P

HEAD_WIDTH = 128
DOCS = 8
MATES = 4
DOCUMENT_SHARE = 4
NEG = -1e30
MESH = pl.DeviceIdType.MESH
FACTOR = HEAD_WIDTH ** (-0.5) * math.log2(math.e)
f32, bf16 = jnp.float32, jnp.bfloat16


def kernel(
    line, span_ref, doc_ref, q_hbm, k_hbm, v_hbm, w_hbm, out_hbm,
    kv, kv_out, q_in, q_out, marks, q_t, slot_of, k_near, v_near, raw, held,
    w_vmem, attn, o_out, partial, outgoing, incoming, kept, ready,
    load_kv, load_q, w_sem, send_kv, send_q, send_o, send_z, recv_kv, recv_q, recv_o, out_send, out_recv, out_sem, turn,
):
    rows = k_hbm.shape[0]
    span_len = rows // 2
    wide = q_hbm.shape[1] // MATES
    group = wide // HEAD_WIDTH
    slots = span_ref.shape[0]
    reach = k_near.shape[1] // span_len
    me = lax.axis_index("cp")
    hd = lax.axis_index("hd")
    z, p = me // MATES, me % MATES
    y, x = p // 2, p % 2
    has_up, has_down = z < line - 1, z > 0
    up, down = me + MATES, me - MATES

    def member(i):
        return (y + (i // 2) * (1 - 2 * y)) * 2 + x + (i % 2) * (1 - 2 * x)

    def mate(i):
        return z * MATES + member(i)

    def columns(i, size):
        return pl.ds(pl.multiple_of(member(i) * size, size), size)

    class kv_load:
        def __init__(self, i, h):
            spot = kv.at[me, h] if i == 0 else kv_out.at[i, h]
            self.copies = [
                pltpu.make_async_copy(
                    (k_hbm, v_hbm)[h].at[s * span_len:(s + 1) * span_len, columns(i, HEAD_WIDTH)],
                    spot.at[s], load_kv.at[i, h, s],
                )
                for s in range(2)
            ]

        def start(self):
            for copy in self.copies:
                copy.start()

        def wait(self):
            for copy in self.copies:
                copy.wait()

    def q_load(i):
        dst = q_in.at[0] if i == 0 else q_out.at[i]
        return pltpu.make_async_copy(q_hbm.at[:, columns(i, wide)], dst, load_q.at[i])

    def w_load(i):
        src = w_hbm.at[pl.ds(pl.multiple_of(member(i) * wide, wide), wide), :]
        return pltpu.make_async_copy(src, w_vmem.at[place[i] * wide:(place[i] + 1) * wide, :], w_sem.at[i])

    def remote(src, dst, send, recv, target):
        return pltpu.make_async_remote_copy(
            src_ref=src, dst_ref=dst, send_sem=send, recv_sem=recv,
            device_id={"cp": target}, device_id_type=MESH,
        )

    def kv_send(i, h):
        return remote(kv_out.at[i, h], kv.at[me, h], send_kv.at[i, h], recv_kv.at[me, h], mate(i))

    def q_send(i):
        return remote(q_out.at[i], q_in.at[i], send_q.at[i], recv_q.at[i], mate(i))

    place = (0, 2, 3, 1)

    def o_send(i, s):
        start = s * span_len if isinstance(s, int) else pl.multiple_of(s * span_len, span_len)
        dst = attn.at[pl.ds(start, span_len), place[i] * wide:(place[i] + 1) * wide]
        return remote(o_out.at[i, s], dst, send_o.at[i, s], recv_o.at[i, s], mate(i))

    def z_send(d, side, i, h, src, target):
        block = kv.at[src, h]
        return remote(block, block, send_z.at[d, side, i, h], recv_kv.at[src, h], target)

    def z_block(d, side, i, src, target):
        return remote(kv.at[src], kv.at[src], send_z.at[d, side, i, 0], recv_kv.at[src, 0], target)

    def arrived(d, src):
        @pl.when(d == 1)
        def _():
            for h in range(2):
                remote(kv.at[src, h], kv.at[src, h], send_z.at[0, 0, 0, h], recv_kv.at[src, h], mate(1)).wait_recv()

        @pl.when(d > 1)
        def _():
            z_block(0, 0, 0, src, mate(1)).wait_recv()

    for i in range(MATES):
        for h in range(2):
            kv_load(i, h).start()
    for i in range(MATES):
        q_load(i).start()

    barrier = pltpu.get_barrier_semaphore()
    for i in range(1, MATES):
        pl.semaphore_signal(barrier, inc=1, device_id={"cp": mate(i)}, device_id_type=MESH)
    pl.semaphore_signal(barrier, inc=1, device_id={"hd": 1 - hd}, device_id_type=MESH)

    @pl.when(has_up)
    def _():
        pl.semaphore_signal(barrier, inc=1, device_id={"cp": up}, device_id_type=MESH)

    @pl.when(has_down)
    def _():
        pl.semaphore_signal(barrier, inc=1, device_id={"cp": down}, device_id_type=MESH)

    for h in range(2):
        kv_load(0, h).wait()
    pl.semaphore_wait(barrier, MATES + has_up.astype(jnp.int32) + has_down.astype(jnp.int32))

    def own_z(i, h, act):
        @pl.when(has_up)
        def _():
            act(z_send(0, 0, i, h, mate(i), up))

        @pl.when(has_down)
        def _():
            act(z_send(0, 1, i, h, mate(i), down))

    def go(copy):
        copy.start()

    def sent(copy):
        copy.wait_send()

    for h in range(2):
        own_z(0, h, go)
    for i in range(1, MATES):
        for h in range(2):
            kv_load(i, h).wait()
            kv_send(i, h).start()

    def send_queries():
        for i in range(1, MATES):
            q_load(i).wait()
            q_send(i).start()

    @pl.when(hd == 0)
    def _():
        send_queries()


    docs = doc_ref[...]
    starts = [jnp.zeros((1, 1), f32)]
    for d in range(1, DOCS):
        starts.append(jnp.sum(jnp.where(docs < d, 1.0, 0.0), keepdims=True))
    starts.append(jnp.full((1, 1), docs.size, f32))
    lane = lax.broadcasted_iota(jnp.int32, (1, HEAD_WIDTH), 1)
    start_row = jnp.full((1, HEAD_WIDTH), 4.0 * docs.size, f32)
    end_row = jnp.full((1, HEAD_WIDTH), 4.0 * docs.size, f32)
    for d in range(DOCS):
        start_row = jnp.where(lane == d, starts[d], start_row)
        end_row = jnp.where(lane == d, starts[d + 1], end_row)
    void = jnp.where(lane == DOCS, NEG, 0.0)
    marks[slots] = jnp.broadcast_to(void, (span_len, HEAD_WIDTH)).astype(bf16)

    def mark(slot, carry):
        key = lax.broadcasted_iota(jnp.int32, (span_len, HEAD_WIDTH), 0)
        key_pos = (span_ref[slot] * span_len + key).astype(f32)
        of_doc = jnp.where((key_pos >= start_row) & (key_pos < end_row), 1.0, 0.0)
        marks[slot] = of_doc.astype(bf16)
        found = 0
        for other in range(slots):
            found = jnp.maximum(found, jnp.where(span_ref[other] == slot, other, 0))
        slot_of[slot] = found
        return carry

    lanes = group * span_len

    def prepare(i):
        at = lax.broadcasted_iota(jnp.int32, (1, lanes), 1) % span_len
        row = lax.broadcasted_iota(jnp.int32, (HEAD_WIDTH, lanes), 0)
        for s in range(2):
            heads = [
                q_in[i, s * span_len:(s + 1) * span_len, h * HEAD_WIDTH:(h + 1) * HEAD_WIDTH]
                for h in range(group)
            ]
            pos = (span_ref[2 * mate(i) + s] * span_len + at).astype(f32)
            extra = jnp.where(row == DOCS, 1.0, 0.0)
            for d in range(DOCS):
                same = (pos >= starts[d]) & (pos < starts[d + 1])
                extra = jnp.where(row == d, jnp.where(same, 0.0, NEG), extra)
            q_t[2 * i + s, :HEAD_WIDTH] = jnp.concatenate(heads, axis=0).T
            q_t[2 * i + s, HEAD_WIDTH:] = extra.astype(bf16)

    turns = [(i, s) for i in (3, 1, 2, 0) for s in range(2)]
    tops = {}

    def collect(j):
        i, s = turns[j]
        last = span_ref[2 * mate(i) + s]
        for k in range(reach):
            span = last - (reach - 1) + k
            slot = slot_of[jnp.maximum(span, 0)]
            cut = slice(k * span_len, (k + 1) * span_len)
            k_near[j % 2, cut, :HEAD_WIDTH] = kv[slot // 2, 0, slot % 2]
            k_near[j % 2, cut, HEAD_WIDTH:] = marks[jnp.where(span >= 0, slot, slots)]
            v_near[j % 3, cut] = kv[slot // 2, 1, slot % 2]

    def score(j):
        i, s = turns[j]
        scores = jnp.dot(k_near[j % 2], q_t[2 * i + s], preferred_element_type=f32)
        edge = (reach - 1) * span_len
        key = lax.broadcasted_iota(jnp.int32, (span_len, lanes), 0)
        at = lax.broadcasted_iota(jnp.int32, (span_len, lanes), 1) % span_len
        corner = jnp.where(key > at, NEG, scores[edge:])
        raw[j % 2, :edge] = scores[:edge]
        raw[j % 2, edge:] = corner
        top = jnp.max(corner, axis=0, keepdims=True)
        tops[j] = jnp.maximum(top, jnp.max(scores[:edge], axis=0, keepdims=True))

    def weigh(j):
        weights = jnp.exp2(raw[j % 2] * FACTOR - tops[j] * FACTOR)
        tops[j] = 1.0 / jnp.sum(weights, axis=0, keepdims=True)
        held[j % 2] = weights.astype(bf16)

    def blend(j):
        i, s = turns[j]
        mixed = jnp.dot(v_near[j % 3].T, held[j % 2], preferred_element_type=f32)
        turned = (mixed * tops[j]).astype(bf16).T
        for h in range(group):
            cut = slice(h * HEAD_WIDTH, (h + 1) * HEAD_WIDTH)
            if i:
                o_out[i, s, :, cut] = turned[h * span_len:(h + 1) * span_len]
            else:
                attn[s * span_len:(s + 1) * span_len, cut] = turned[h * span_len:(h + 1) * span_len]
        if i:
            o_send(i, s).start()

    ways = ((0, -1, z, has_up, up), (1, 1, line - 1 - z, has_down, down))

    def forward(d, i):
        for side, sign, last, more, target in ways:
            src = (z + sign * d) * MATES + member(i)

            @pl.when(d <= last)
            def _():
                arrived(d, src)

                @pl.when(more)
                def _():
                    z_block(d, side, i, src, target).start()

    def await_turn():
        for side, sign, last, more, target in ways:

            @pl.when(jnp.minimum(last, more.astype(jnp.int32)) > 0)
            def _():
                pl.semaphore_wait(turn.at[side], 1)

    def give_turn(d):
        for side, sign, last, more, target in ways:

            @pl.when((last == d) & more)
            def _():
                pl.semaphore_signal(turn.at[side], inc=1, device_id={"hd": 1 - hd}, device_id_type=MESH)

    def drained(d, i):
        for side, sign, last, more, target in ways:
            src = (z + sign * d) * MATES + member(i)

            @pl.when((d <= last) & more)
            def _():
                z_block(d, side, i, src, target).wait_send()

    def pass_on(i, h):
        src = mate(i)
        remote(kv.at[src, h], kv.at[src, h], send_z.at[0, 0, 0, h], recv_kv.at[src, h], src).wait_recv()
        own_z(i, h, go)

    def relay(n, carry):
        forward(n // MATES + 1, n % MATES)
        return carry

    for h in range(2):
        pass_on(1, h)
        pass_on(2, h)
    for i in range(MATES):
        w_load(i).start()
    for h in range(2):
        pass_on(3, h)

    @pl.when(hd == 0)
    def _():
        def lead(n, carry):
            relay(n, carry)

            @pl.when(n % MATES == MATES - 1)
            def _():
                give_turn(n // MATES + 1)

            return carry

        lax.fori_loop(0, (line - 1) * MATES, lead, 0)

    @pl.when(hd == 1)
    def _():
        send_queries()

    lax.fori_loop(0, slots, mark, 0)
    q_load(0).wait()
    prepare(0)
    for i in range(1, MATES):
        q_send(i).wait_recv()
        prepare(i)

    @pl.when(hd == 1)
    def _():
        await_turn()
        lax.fori_loop(0, (line - 1) * MATES, relay, 0)

    for t in range(len(turns) + 2):
        if t < len(turns):
            collect(t)
            score(t)
        if 1 <= t <= len(turns):
            weigh(t - 1)
        if t >= 2:
            blend(t - 2)

    for i in range(MATES):
        w_load(i).wait()

    half = rows // 2
    count, width = outgoing.shape[0], outgoing.shape[2]

    def hand_over(n):
        return pltpu.make_async_remote_copy(
            src_ref=outgoing.at[n], dst_ref=incoming.at[n], send_sem=out_send.at[n],
            recv_sem=out_recv.at[n], device_id={"hd": 1 - hd}, device_id_type=MESH,
        )

    def store(n):
        return pltpu.make_async_copy(
            ready.at[n], out_hbm.at[:, n * width:(n + 1) * width], out_sem.at[n]
        )

    def project(n, rest, lines):
        cut = slice(2 * wide, 4 * wide) if rest else slice(0, 2 * wide)
        return jnp.dot(attn[lines, cut], w_vmem[cut, n * width:(n + 1) * width], preferred_element_type=f32)

    for s in range(2):
        o_send(3, s).wait_recv()
    for n in range(count):
        partial[n] = project(n, False, slice(None))
    theirs, ours = [pl.ds(pl.multiple_of(s * half, half), half) for s in (1 - hd, hd)]
    for i in (1, 2):
        o_send(i, 1 - hd).wait_recv()
    for n in range(count):
        outgoing[n] = (partial[n, theirs] + project(n, True, theirs)).astype(bf16)
        hand_over(n).start()
    for i in (1, 2):
        o_send(i, hd).wait_recv()
    for n in range(count):
        kept[n] = partial[n, ours] + project(n, True, ours)
    for n in range(count):
        hand_over(n).wait_recv()
        ready[n] = (kept[n] + incoming[n].astype(f32)).astype(bf16)
        store(n).start()
    for n in range(count):
        store(n).wait()

    for n in range(count):
        hand_over(n).wait_send()
    for i in range(1, MATES):
        for h in range(2):
            kv_send(i, h).wait_send()
        q_send(i).wait_send()
        for s in range(2):
            o_send(i, s).wait_send()
    for i in range(MATES):
        for h in range(2):
            own_z(i, h, sent)

    def drain(n, carry):
        drained(n // MATES + 1, n % MATES)
        return carry

    lax.fori_loop(0, (line - 1) * MATES, drain, 0)


def local(cp, queries, keys, values, span_table, doc_ids, out_weight):
    rows = queries.shape[0]
    kv_heads = keys.shape[1] // HEAD_WIDTH
    wide = queries.shape[1] // kv_heads
    slots = span_table.shape[0]
    span_len = rows // 2
    lanes = wide // HEAD_WIDTH * span_len
    near = (slots // DOCUMENT_SHARE + 1) * span_len
    line = cp // MATES
    model = out_weight.shape[1]
    count = 8
    width = model // count
    half = rows // 2
    vmem, hbm = pltpu.VMEM, pl.ANY
    spec = lambda space: pl.BlockSpec(memory_space=space)
    dma = pltpu.SemaphoreType.DMA
    return pl.pallas_call(
        functools.partial(kernel, line),
        out_shape=jax.ShapeDtypeStruct((half, model), bf16),
        in_specs=[spec(pltpu.SMEM), spec(vmem), spec(hbm), spec(hbm), spec(hbm), spec(hbm)],
        out_specs=spec(hbm),
        scratch_shapes=[
            vmem((cp, 2, 2, span_len, HEAD_WIDTH), bf16),
            vmem((MATES, 2, 2, span_len, HEAD_WIDTH), bf16),
            vmem((MATES, rows, wide), bf16),
            vmem((MATES, rows, wide), bf16),
            vmem((slots + 1, span_len, HEAD_WIDTH), bf16),
            vmem((2 * MATES, 2 * HEAD_WIDTH, lanes), bf16),
            pltpu.SMEM((slots,), jnp.int32),
            vmem((2, near, 2 * HEAD_WIDTH), bf16),
            vmem((3, near, HEAD_WIDTH), bf16),
            vmem((2, near, lanes), f32),
            vmem((2, near, lanes), bf16),
            vmem(out_weight.shape, bf16),
            vmem((rows, MATES * wide), bf16),
            vmem((MATES, 2, span_len, wide), bf16),
            vmem((count, rows, width), f32),
            vmem((count, half, width), bf16),
            vmem((count, half, width), bf16),
            vmem((count, half, width), f32),
            vmem((count, half, width), bf16),
            dma((MATES, 2, 2)), dma((MATES,)), dma((MATES,)), dma((MATES, 2)), dma((MATES,)), dma((MATES, 2)),
            dma((line, 2, MATES, 2)), dma((cp, 2)), dma((MATES,)), dma((MATES, 2)), dma((count,)), dma((count,)), dma((count,)),
            pltpu.SemaphoreType.REGULAR((2,)),
        ],
        compiler_params=pltpu.CompilerParams(
            collective_id=0, has_side_effects=True, vmem_limit_bytes=62 * 2 ** 20,
        ),
    )(span_table, doc_ids.reshape(-1, 128), queries, keys, values, out_weight)


def solution(mesh):
    return jax.shard_map(
        functools.partial(local, mesh.shape["cp"]),
        mesh=mesh,
        in_specs=(P("cp", "hd"), P("cp", "hd"), P("cp", "hd"), P(), P(), P("hd", None)),
        out_specs=P(("cp", "hd"), None),
        check_vma=False,
    )
```

```python
import functools
import math

import jax
import jax.numpy as jnp
from jax import lax
from jax.experimental import pallas as pl
from jax.experimental.pallas import tpu as pltpu
from jax.sharding import PartitionSpec as P

HEAD_WIDTH = 128
DOCS = 8
MATES = 4
DOCUMENT_SHARE = 4
NEG = -1e30
MESH = pl.DeviceIdType.MESH
FACTOR = HEAD_WIDTH ** (-0.5) * math.log2(math.e)
f32, bf16 = jnp.float32, jnp.bfloat16


def kernel(
    line, span_hbm, doc_hbm, q_hbm, k_hbm, v_hbm, w_hbm, out_hbm,
    kv, kv_out, q_in, q_out, marks, q_t, span_ref, doc_ref, slot_of, k_near, v_near, raw, held,
    w_vmem, attn, o_out, partial, outgoing, incoming, kept, ready,
    load_kv, load_q, w_sem, send_kv, send_q, send_o, send_z, recv_kv, recv_q, recv_o, out_send, out_recv, out_sem, table_sem, turn,
):
    rows = k_hbm.shape[0]
    span_len = rows // 2
    wide = q_hbm.shape[1] // MATES
    group = wide // HEAD_WIDTH
    slots = span_hbm.shape[0]
    reach = k_near.shape[1] // span_len
    me = lax.axis_index("cp")
    hd = lax.axis_index("hd")
    z, p = me // MATES, me % MATES
    y, x = p // 2, p % 2
    has_up, has_down = z < line - 1, z > 0
    up, down = me + MATES, me - MATES

    def member(i):
        return (y + (i // 2) * (1 - 2 * y)) * 2 + x + (i % 2) * (1 - 2 * x)

    def mate(i):
        return z * MATES + member(i)

    def columns(i, size):
        return pl.ds(pl.multiple_of(member(i) * size, size), size)

    class kv_load:
        def __init__(self, i, h):
            spot = kv.at[me, h] if i == 0 else kv_out.at[i, h]
            self.copies = [
                pltpu.make_async_copy(
                    (k_hbm, v_hbm)[h].at[s * span_len:(s + 1) * span_len, columns(i, HEAD_WIDTH)],
                    spot.at[s], load_kv.at[i, h, s],
                )
                for s in range(2)
            ]

        def start(self):
            for copy in self.copies:
                copy.start()

        def wait(self):
            for copy in self.copies:
                copy.wait()

    def q_load(i):
        dst = q_in.at[0] if i == 0 else q_out.at[i]
        return pltpu.make_async_copy(q_hbm.at[:, columns(i, wide)], dst, load_q.at[i])

    def w_load(i):
        src = w_hbm.at[pl.ds(pl.multiple_of(member(i) * wide, wide), wide), :]
        return pltpu.make_async_copy(src, w_vmem.at[place[i] * wide:(place[i] + 1) * wide, :], w_sem.at[i])

    def remote(src, dst, send, recv, target):
        return pltpu.make_async_remote_copy(
            src_ref=src, dst_ref=dst, send_sem=send, recv_sem=recv,
            device_id={"cp": target}, device_id_type=MESH,
        )

    def kv_send(i, h):
        return remote(kv_out.at[i, h], kv.at[me, h], send_kv.at[i, h], recv_kv.at[me, h], mate(i))

    def q_send(i):
        return remote(q_out.at[i], q_in.at[i], send_q.at[i], recv_q.at[i], mate(i))

    place = (0, 2, 3, 1)

    def o_send(i, s):
        start = s * span_len if isinstance(s, int) else pl.multiple_of(s * span_len, span_len)
        dst = attn.at[pl.ds(start, span_len), place[i] * wide:(place[i] + 1) * wide]
        return remote(o_out.at[i, s], dst, send_o.at[i, s], recv_o.at[i, s], mate(i))

    def z_send(d, side, i, h, src, target):
        block = kv.at[src, h]
        return remote(block, block, send_z.at[d, side, i, h], recv_kv.at[src, h], target)

    def z_block(d, side, i, src, target):
        return remote(kv.at[src], kv.at[src], send_z.at[d, side, i, 0], recv_kv.at[src, 0], target)

    def arrived(d, src):
        @pl.when(d == 1)
        def _():
            for h in range(2):
                remote(kv.at[src, h], kv.at[src, h], send_z.at[0, 0, 0, h], recv_kv.at[src, h], mate(1)).wait_recv()

        @pl.when(d > 1)
        def _():
            z_block(0, 0, 0, src, mate(1)).wait_recv()

    tables = [
        pltpu.make_async_copy(span_hbm, span_ref, table_sem.at[0]),
        pltpu.make_async_copy(doc_hbm, doc_ref, table_sem.at[1]),
    ]
    for i in range(MATES):
        for h in range(2):
            kv_load(i, h).start()
    for table in tables:
        table.start()
    for i in range(MATES):
        q_load(i).start()

    barrier = pltpu.get_barrier_semaphore()
    for i in range(1, MATES):
        pl.semaphore_signal(barrier, inc=1, device_id={"cp": mate(i)}, device_id_type=MESH)
    pl.semaphore_signal(barrier, inc=1, device_id={"hd": 1 - hd}, device_id_type=MESH)

    @pl.when(has_up)
    def _():
        pl.semaphore_signal(barrier, inc=1, device_id={"cp": up}, device_id_type=MESH)

    @pl.when(has_down)
    def _():
        pl.semaphore_signal(barrier, inc=1, device_id={"cp": down}, device_id_type=MESH)

    for h in range(2):
        kv_load(0, h).wait()
    pl.semaphore_wait(barrier, MATES + has_up.astype(jnp.int32) + has_down.astype(jnp.int32))

    def own_z(i, h, act):
        @pl.when(has_up)
        def _():
            act(z_send(0, 0, i, h, mate(i), up))

        @pl.when(has_down)
        def _():
            act(z_send(0, 1, i, h, mate(i), down))

    def go(copy):
        copy.start()

    def sent(copy):
        copy.wait_send()

    for h in range(2):
        own_z(0, h, go)
    for i in range(1, MATES):
        for h in range(2):
            kv_load(i, h).wait()
            kv_send(i, h).start()

    def send_queries():
        for i in range(1, MATES):
            q_load(i).wait()
            q_send(i).start()

    @pl.when(hd == 0)
    def _():
        send_queries()


    for table in tables:
        table.wait()
    docs = doc_ref[...]
    starts = [jnp.zeros((1, 1), f32)]
    for d in range(1, DOCS):
        starts.append(jnp.sum(jnp.where(docs < d, 1.0, 0.0), keepdims=True))
    starts.append(jnp.full((1, 1), docs.size, f32))
    lane = lax.broadcasted_iota(jnp.int32, (1, HEAD_WIDTH), 1)
    start_row = jnp.full((1, HEAD_WIDTH), 4.0 * docs.size, f32)
    end_row = jnp.full((1, HEAD_WIDTH), 4.0 * docs.size, f32)
    for d in range(DOCS):
        start_row = jnp.where(lane == d, starts[d], start_row)
        end_row = jnp.where(lane == d, starts[d + 1], end_row)
    void = jnp.where(lane == DOCS, NEG, 0.0)
    marks[slots] = jnp.broadcast_to(void, (span_len, HEAD_WIDTH)).astype(bf16)

    def mark(slot, carry):
        key = lax.broadcasted_iota(jnp.int32, (span_len, HEAD_WIDTH), 0)
        key_pos = (span_ref[slot] * span_len + key).astype(f32)
        of_doc = jnp.where((key_pos >= start_row) & (key_pos < end_row), 1.0, 0.0)
        marks[slot] = of_doc.astype(bf16)
        found = 0
        for other in range(slots):
            found = jnp.maximum(found, jnp.where(span_ref[other] == slot, other, 0))
        slot_of[slot] = found
        return carry

    lanes = group * span_len

    def prepare(i):
        at = lax.broadcasted_iota(jnp.int32, (1, lanes), 1) % span_len
        row = lax.broadcasted_iota(jnp.int32, (HEAD_WIDTH, lanes), 0)
        for s in range(2):
            heads = [
                q_in[i, s * span_len:(s + 1) * span_len, h * HEAD_WIDTH:(h + 1) * HEAD_WIDTH]
                for h in range(group)
            ]
            pos = (span_ref[2 * mate(i) + s] * span_len + at).astype(f32)
            extra = jnp.where(row == DOCS, 1.0, 0.0)
            for d in range(DOCS):
                same = (pos >= starts[d]) & (pos < starts[d + 1])
                extra = jnp.where(row == d, jnp.where(same, 0.0, NEG), extra)
            q_t[2 * i + s, :HEAD_WIDTH] = jnp.concatenate(heads, axis=0).T
            q_t[2 * i + s, HEAD_WIDTH:] = extra.astype(bf16)

    turns = [(i, s) for i in (3, 1, 2, 0) for s in range(2)]
    tops = {}

    def collect(j):
        i, s = turns[j]
        last = span_ref[2 * mate(i) + s]
        for k in range(reach):
            span = last - (reach - 1) + k
            slot = slot_of[jnp.maximum(span, 0)]
            cut = slice(k * span_len, (k + 1) * span_len)
            k_near[j % 2, cut, :HEAD_WIDTH] = kv[slot // 2, 0, slot % 2]
            k_near[j % 2, cut, HEAD_WIDTH:] = marks[jnp.where(span >= 0, slot, slots)]
            v_near[j % 3, cut] = kv[slot // 2, 1, slot % 2]

    def score(j):
        i, s = turns[j]
        scores = jnp.dot(k_near[j % 2], q_t[2 * i + s], preferred_element_type=f32)
        edge = (reach - 1) * span_len
        key = lax.broadcasted_iota(jnp.int32, (span_len, lanes), 0)
        at = lax.broadcasted_iota(jnp.int32, (span_len, lanes), 1) % span_len
        corner = jnp.where(key > at, NEG, scores[edge:])
        raw[j % 2, :edge] = scores[:edge]
        raw[j % 2, edge:] = corner
        top = jnp.max(corner, axis=0, keepdims=True)
        tops[j] = jnp.maximum(top, jnp.max(scores[:edge], axis=0, keepdims=True))

    def weigh(j):
        weights = jnp.exp2(raw[j % 2] * FACTOR - tops[j] * FACTOR)
        tops[j] = 1.0 / jnp.sum(weights, axis=0, keepdims=True)
        held[j % 2] = weights.astype(bf16)

    def blend(j):
        i, s = turns[j]
        mixed = jnp.dot(v_near[j % 3].T, held[j % 2], preferred_element_type=f32)
        turned = (mixed * tops[j]).astype(bf16).T
        for h in range(group):
            cut = slice(h * HEAD_WIDTH, (h + 1) * HEAD_WIDTH)
            if i:
                o_out[i, s, :, cut] = turned[h * span_len:(h + 1) * span_len]
            else:
                attn[s * span_len:(s + 1) * span_len, cut] = turned[h * span_len:(h + 1) * span_len]
        if i:
            o_send(i, s).start()

    ways = ((0, -1, z, has_up, up), (1, 1, line - 1 - z, has_down, down))

    def forward(d, i):
        for side, sign, last, more, target in ways:
            src = (z + sign * d) * MATES + member(i)

            @pl.when(d <= last)
            def _():
                arrived(d, src)

                @pl.when(more)
                def _():
                    z_block(d, side, i, src, target).start()

    def await_turn():
        for side, sign, last, more, target in ways:

            @pl.when(jnp.minimum(last, more.astype(jnp.int32)) > 0)
            def _():
                pl.semaphore_wait(turn.at[side], 1)

    def give_turn(d):
        for side, sign, last, more, target in ways:

            @pl.when((last == d) & more)
            def _():
                pl.semaphore_signal(turn.at[side], inc=1, device_id={"hd": 1 - hd}, device_id_type=MESH)

    def drained(d, i):
        for side, sign, last, more, target in ways:
            src = (z + sign * d) * MATES + member(i)

            @pl.when((d <= last) & more)
            def _():
                z_block(d, side, i, src, target).wait_send()

    def pass_on(i, h):
        src = mate(i)
        remote(kv.at[src, h], kv.at[src, h], send_z.at[0, 0, 0, h], recv_kv.at[src, h], src).wait_recv()
        own_z(i, h, go)

    def relay(n, carry):
        forward(n // MATES + 1, n % MATES)
        return carry

    for h in range(2):
        pass_on(1, h)
        pass_on(2, h)
    for i in range(MATES):
        w_load(i).start()
    for h in range(2):
        pass_on(3, h)

    @pl.when(hd == 0)
    def _():
        def lead(n, carry):
            relay(n, carry)

            @pl.when(n % MATES == MATES - 1)
            def _():
                give_turn(n // MATES + 1)

            return carry

        lax.fori_loop(0, (line - 1) * MATES, lead, 0)

    @pl.when(hd == 1)
    def _():
        send_queries()

    lax.fori_loop(0, slots, mark, 0)
    q_load(0).wait()
    prepare(0)
    for i in range(1, MATES):
        q_send(i).wait_recv()
        prepare(i)

    @pl.when(hd == 1)
    def _():
        await_turn()
        lax.fori_loop(0, (line - 1) * MATES, relay, 0)

    for t in range(len(turns) + 2):
        if t < len(turns):
            collect(t)
            score(t)
        if 1 <= t <= len(turns):
            weigh(t - 1)
        if t >= 2:
            blend(t - 2)

    for i in range(MATES):
        w_load(i).wait()

    half = rows // 2
    count, width = outgoing.shape[0], outgoing.shape[2]

    def hand_over(n):
        return pltpu.make_async_remote_copy(
            src_ref=outgoing.at[n], dst_ref=incoming.at[n], send_sem=out_send.at[n],
            recv_sem=out_recv.at[n], device_id={"hd": 1 - hd}, device_id_type=MESH,
        )

    def store(n):
        return pltpu.make_async_copy(
            ready.at[n], out_hbm.at[:, n * width:(n + 1) * width], out_sem.at[n]
        )

    def project(n, rest, lines):
        cut = slice(2 * wide, 4 * wide) if rest else slice(0, 2 * wide)
        return jnp.dot(attn[lines, cut], w_vmem[cut, n * width:(n + 1) * width], preferred_element_type=f32)

    for s in range(2):
        o_send(3, s).wait_recv()
    for n in range(count):
        partial[n] = project(n, False, slice(None))
    theirs, ours = [pl.ds(pl.multiple_of(s * half, half), half) for s in (1 - hd, hd)]
    for i in (1, 2):
        o_send(i, 1 - hd).wait_recv()
    for n in range(count):
        outgoing[n] = (partial[n, theirs] + project(n, True, theirs)).astype(bf16)
        hand_over(n).start()
    for i in (1, 2):
        o_send(i, hd).wait_recv()
    for n in range(count):
        kept[n] = partial[n, ours] + project(n, True, ours)
    for n in range(count):
        hand_over(n).wait_recv()
        ready[n] = (kept[n] + incoming[n].astype(f32)).astype(bf16)
        store(n).start()
    for n in range(count):
        store(n).wait()

    for n in range(count):
        hand_over(n).wait_send()
    for i in range(1, MATES):
        for h in range(2):
            kv_send(i, h).wait_send()
        q_send(i).wait_send()
        for s in range(2):
            o_send(i, s).wait_send()
    for i in range(MATES):
        for h in range(2):
            own_z(i, h, sent)

    def drain(n, carry):
        drained(n // MATES + 1, n % MATES)
        return carry

    lax.fori_loop(0, (line - 1) * MATES, drain, 0)


def local(cp, queries, keys, values, span_table, doc_ids, out_weight):
    rows = queries.shape[0]
    kv_heads = keys.shape[1] // HEAD_WIDTH
    wide = queries.shape[1] // kv_heads
    slots = span_table.shape[0]
    span_len = rows // 2
    lanes = wide // HEAD_WIDTH * span_len
    near = (slots // DOCUMENT_SHARE + 1) * span_len
    line = cp // MATES
    model = out_weight.shape[1]
    count = 8
    width = model // count
    half = rows // 2
    vmem, hbm = pltpu.VMEM, pl.ANY
    spec = lambda space: pl.BlockSpec(memory_space=space)
    dma = pltpu.SemaphoreType.DMA
    return pl.pallas_call(
        functools.partial(kernel, line),
        out_shape=jax.ShapeDtypeStruct((half, model), bf16),
        in_specs=[spec(hbm), spec(hbm), spec(hbm), spec(hbm), spec(hbm), spec(hbm)],
        out_specs=spec(hbm),
        scratch_shapes=[
            vmem((cp, 2, 2, span_len, HEAD_WIDTH), bf16),
            vmem((MATES, 2, 2, span_len, HEAD_WIDTH), bf16),
            vmem((MATES, rows, wide), bf16),
            vmem((MATES, rows, wide), bf16),
            vmem((slots + 1, span_len, HEAD_WIDTH), bf16),
            vmem((2 * MATES, 2 * HEAD_WIDTH, lanes), bf16),
            pltpu.SMEM((slots,), jnp.int32),
            vmem((doc_ids.shape[0] // 128, 128), jnp.int32),
            pltpu.SMEM((slots,), jnp.int32),
            vmem((2, near, 2 * HEAD_WIDTH), bf16),
            vmem((3, near, HEAD_WIDTH), bf16),
            vmem((2, near, lanes), f32),
            vmem((2, near, lanes), bf16),
            vmem(out_weight.shape, bf16),
            vmem((rows, MATES * wide), bf16),
            vmem((MATES, 2, span_len, wide), bf16),
            vmem((count, rows, width), f32),
            vmem((count, half, width), bf16),
            vmem((count, half, width), bf16),
            vmem((count, half, width), f32),
            vmem((count, half, width), bf16),
            dma((MATES, 2, 2)), dma((MATES,)), dma((MATES,)), dma((MATES, 2)), dma((MATES,)), dma((MATES, 2)),
            dma((line, 2, MATES, 2)), dma((cp, 2)), dma((MATES,)), dma((MATES, 2)), dma((count,)), dma((count,)), dma((count,)), dma((2,)),
            pltpu.SemaphoreType.REGULAR((2,)),
        ],
        compiler_params=pltpu.CompilerParams(
            collective_id=0, has_side_effects=True, vmem_limit_bytes=62 * 2 ** 20,
        ),
    )(span_table, doc_ids.reshape(-1, 128), queries, keys, values, out_weight)


def solution(mesh):
    return jax.shard_map(
        functools.partial(local, mesh.shape["cp"]),
        mesh=mesh,
        in_specs=(P("cp", "hd"), P("cp", "hd"), P("cp", "hd"), P(), P(), P("hd", None)),
        out_specs=P(("cp", "hd"), None),
        check_vma=False,
    )
```
